32 devices in a mesh: dp: 4 (over z), expert: 4 (over y, core), tensor: 2 (over x).
Axes of the slice: x: 2, y: 2, z: 4, core: 2. Of those that a mesh axis runs over, the one named last changes fastest.
Arguments:
- hidden: bfloat16 [2048, 6144], P(('dp', 'expert'), 'tensor'), may hold values from -6 to 6
- expert_ids: int32 [2048, 8], P(('dp', 'expert')), may hold values from 0 to 383, as said below
- gate_fixed: int32 [2048, 8], P(('dp', 'expert')), may hold values from 4096 to 65535
- slot_expert: int32 [16], replicated, may hold values from 0 to 383, as said below
- expert_in: bfloat16 [16, 6144, 2, 1024], P(('dp', 'expert'), 'tensor'), may hold values from -1 to 1, as said below
- expert_out: bfloat16 [16, 1024, 6144], P(('dp', 'expert'), None, 'tensor'), may hold values from -1 to 1, as said below
- shared_in: bfloat16 [6144, 2, 1024], P('tensor', None, 'dp'), may hold values from -0.078125 to 0.078125
- shared_out: bfloat16 [1024, 6144], P('dp', 'tensor'), may hold values from -0.1875 to 0.1875
Outputs:
- mixed: bfloat16 [2048, 6144], P(('dp', 'expert'), 'tensor')
The draws below stay inside these ranges and needn't reach their ends.
Inputs may be any that keep to these rules, and one draw needn't show every extreme that they name: `expert_ids`: each row names 8 different experts. `slot_expert`: 14 different experts fill the 16 slots; 2 of them hold two slots each, the others one. `expert_in`: slots that hold the same expert hold the same weights. `expert_out`: slots that hold the same expert hold the same weights.
All inputs are finite; a program needn't handle non-finite values.
Results may differ from the reference program's by a relative error of at most 0.006.
Values may be sent and summed in bfloat16 or wider, within the bound.
A program may use at most 192 MiB of HBM per device.

```python
import jax
import jax.numpy as jnp
from jax import lax

D = 6144
FF_E = 1024
FF_S = 1024
EXPERTS = 384
TOPK = 8
CAP = 4
TOK_DEV = 128
SLOTS = 16
REPL = 2
WIN = 14
TOKENS = 2048


def routing_plan(key):
    base = jax.random.fold_in(key, 4242)
    key_bias, key_noise, key_pick, key_perm = jax.random.split(base, 4)
    order = jnp.arange(EXPERTS, dtype=jnp.int32)
    level = jax.random.randint(key_bias, (EXPERTS,), 0, 8, dtype=jnp.int32)
    bias = level * level
    noise = jax.random.randint(key_noise, (TOKENS, EXPERTS), 0, 1024, dtype=jnp.int32)
    score = (noise + bias[None, :]) * EXPERTS + order[None, :]
    _, chosen = lax.top_k(score, TOPK)
    pick = jax.random.randint(key_pick, (EXPERTS,), 0, 1 << 20, dtype=jnp.int32) * EXPERTS + order
    ends = (order == 0) | (order == EXPERTS - 1)
    pick = jnp.where(ends, (1 << 21) * EXPERTS + order, pick).astype(jnp.int32)
    _, resident = lax.top_k(pick, WIN)
    heat = bias[resident] * EXPERTS + resident
    _, hot_place = lax.top_k(heat, REPL)
    entries = jnp.concatenate([jnp.arange(WIN, dtype=jnp.int32), hot_place.astype(jnp.int32)])
    shuffle = jax.random.permutation(key_perm, SLOTS)
    slot_resident = entries[shuffle]
    return (chosen.astype(jnp.int32), resident[slot_resident].astype(jnp.int32), slot_resident)


def expert_weights(key, salt, shape, fan_in):
    _, _, slot_resident = routing_plan(key)
    weight_key = jax.random.fold_in(key, salt)
    factor = fan_in ** (-0.5)

    def one_slot(resident_index):
        values = jax.random.truncated_normal(jax.random.fold_in(weight_key, resident_index), -4.0, 4.0, shape, jnp.float32)
        return (values * factor).astype(jnp.bfloat16)
    return lax.map(one_slot, slot_resident)


def draw_expert_ids(key, part):
    return routing_plan(key)[0]


def draw_slot_expert(key, part):
    return routing_plan(key)[1]


def draw_expert_in(key, part):
    return expert_weights(key, 17, (D, 2, FF_E), D)


def draw_expert_out(key, part):
    return expert_weights(key, 29, (FF_E, D), FF_E)


def touch_ends(array, own_key, low, high):
    dims = array.shape
    place = [jax.random.randint(jax.random.fold_in(own_key, axis), (), 0, dims[axis]) for axis in range(len(dims))]
    array = array.at[tuple(place)].set(low)
    longest = dims.index(max(dims))
    place[longest] = (place[longest] + 1) % dims[longest]
    return array.at[tuple(place)].set(high)


def steps_of(own_key, shape, cuts, smallest, high):
    def one(position, parts):
        heights = jax.random.uniform(jax.random.fold_in(jax.random.fold_in(own_key, 6), position), (parts,), jnp.float32, smallest / len(cuts), high / len(cuts))
        return jnp.repeat(jnp.exp(heights), shape[position] // parts).reshape((-1,) + (1,) * (len(shape) - position - 1))

    loudness = one(*cuts[0])
    for cut in cuts[1:]:
        loudness = loudness * one(*cut)
    return loudness


def scatter_about(rng, shape, width, bound, shards=(), kind=jnp.bfloat16):
    drawn = width * jax.random.normal(rng, shape, jnp.float32)
    if shards:
        drawn = drawn * steps_of(rng, shape, shards, -0.22, 0.18)
    return jnp.clip(drawn, -bound, bound).astype(kind)


def setup_inputs(seed: int = 0) -> dict:
    keys = jax.random.split(jax.random.key(seed), 9)
    hidden = scatter_about(keys[0], (TOKENS, D), 1.0, 6.0, ((0, 16), (1, 2)))
    expert_ids = draw_expert_ids(jax.random.fold_in(keys[8], 71), 0)
    gate_fixed = touch_ends(jax.random.randint(keys[2], (TOKENS, TOPK), 4096, 65536), jax.random.fold_in(keys[2], 1), 4096, 65535).astype(jnp.int32)
    slot_expert = draw_slot_expert(jax.random.fold_in(keys[8], 71), 0)
    expert_in = draw_expert_in(jax.random.fold_in(keys[8], 71), 0)
    expert_out = draw_expert_out(jax.random.fold_in(keys[8], 71), 0)
    shared_in = scatter_about(keys[6], (D, 2, FF_S), D ** -0.5, 0.078125, ((0, 2), (2, 4)))
    shared_out = scatter_about(keys[7], (FF_S, D), FF_S ** -0.5, 0.1875, ((0, 4), (1, 2)))
    return dict(hidden=hidden, expert_ids=expert_ids, gate_fixed=gate_fixed, slot_expert=slot_expert, expert_in=expert_in, expert_out=expert_out, shared_in=shared_in, shared_out=shared_out)


gate_scale = 1.0 / 65536.0


def swiglu(pre):
    return (jax.nn.silu(pre[:, 0, :]) * pre[:, 1, :]).astype(jnp.bfloat16)


def route_plan(chosen, row_rank, slot_expert):
    slot_count = slot_expert.shape[0]
    slot_iota = jnp.arange(slot_count, dtype=jnp.int32)[:, None]
    owns = slot_expert[:, None] == jnp.arange(chosen.shape[2], dtype=jnp.int32)[None, :]
    home = jnp.min(jnp.where(owns, slot_iota, slot_count), axis=0).astype(jnp.int32)
    spare = jnp.min(jnp.where(owns & (slot_iota != home[None, :]), slot_iota, slot_count), axis=0).astype(jnp.int32)
    home_of = jnp.sum(jnp.where(chosen, home[None, None, :], 0), axis=2).astype(jnp.int32)
    spare_of = jnp.sum(jnp.where(chosen, spare[None, None, :], 0), axis=2).astype(jnp.int32)
    first = row_rank < CAP
    spill = (row_rank >= CAP) & (row_rank < 2 * CAP) & (spare_of < slot_count)
    target = jnp.where(first, home_of, jnp.where(spill, spare_of, slot_count)).astype(jnp.int32)
    slot_row = jnp.where(first, row_rank, row_rank - CAP).astype(jnp.int32)
    return target, slot_row


def reference(hidden, expert_ids, gate_fixed, slot_expert, expert_in, expert_out, shared_in, shared_out):
    tokens_all = hidden.shape[0]
    slot_count = slot_expert.shape[0]
    blocks = tokens_all // TOK_DEV
    experts_iota = jnp.arange(EXPERTS, dtype=jnp.int32)
    chosen = expert_ids[:, :, None] == experts_iota[None, None, :]
    picked = jnp.any(chosen, axis=1).astype(jnp.int32).reshape(blocks, TOK_DEV, EXPERTS)
    before = (jnp.cumsum(picked, axis=1) - picked).astype(jnp.int32).reshape(tokens_all, EXPERTS)
    row_rank = jnp.sum(jnp.where(chosen, before[:, None, :], 0), axis=2).astype(jnp.int32)
    target, slot_row = route_plan(chosen, row_rank, slot_expert)
    token_iota = jnp.arange(tokens_all, dtype=jnp.int32)
    token_block = token_iota // TOK_DEV
    buffer_size = slot_count * blocks * CAP
    flat = jnp.where(target < slot_count, (target * blocks + token_block[:, None]) * CAP + slot_row, buffer_size).astype(jnp.int32)
    owner = jnp.broadcast_to(token_iota[:, None], flat.shape).astype(jnp.int32)
    table = jnp.full((buffer_size + 1,), tokens_all, jnp.int32).at[flat.reshape(-1)].set(owner.reshape(-1))
    table = table[:buffer_size].reshape(slot_count, blocks * CAP)
    padded = jnp.concatenate([hidden, jnp.zeros((1, D), hidden.dtype)], axis=0)

    def expert_pass(item):
        rows_index, weight_in, weight_out = item
        rows = padded[rows_index]
        pre = jnp.dot(rows, weight_in.reshape(D, 2 * FF_E), preferred_element_type=jnp.float32).reshape(-1, 2, FF_E)
        return jnp.dot(swiglu(pre), weight_out, preferred_element_type=jnp.float32).astype(jnp.bfloat16)

    answers = lax.map(expert_pass, (table, expert_in, expert_out)).reshape(buffer_size, D)
    answers = jnp.concatenate([answers, jnp.zeros((1, D), answers.dtype)], axis=0)
    gates = gate_fixed.astype(jnp.float32) * gate_scale
    routed = jnp.zeros((tokens_all, D), jnp.float32)
    for column in range(TOPK):
        routed = routed + gates[:, column:column + 1] * answers[flat[:, column]].astype(jnp.float32)
    shared_pre = jnp.dot(hidden, shared_in.reshape(D, 2 * FF_S), preferred_element_type=jnp.float32).reshape(-1, 2, FF_S)
    shared = jnp.dot(swiglu(shared_pre), shared_out, preferred_element_type=jnp.float32)
    return (shared + routed).astype(jnp.bfloat16)
```

```python
import jax
import jax.numpy as jnp
from jax import lax
from jax.sharding import PartitionSpec as P

CAP = 4
CHUNKS = 2
gate_scale = 1.0 / 65536.0
BF = jnp.bfloat16
F32 = jnp.float32


def swiglu(gate, up):
    return (jax.nn.silu(gate) * up).astype(BF)


def across_tensor(partial, tensor_size):
    sent = partial.astype(BF)
    total = partial
    for shift in range(1, tensor_size):
        ring = [(i, (i + shift) % tensor_size) for i in range(tensor_size)]
        total = total + lax.ppermute(sent, "tensor", ring).astype(F32)
    return total


def slot_plan(expert_ids, gate_fixed, slot_expert):
    tok_rows, topk_count = expert_ids.shape
    slot_count = slot_expert.shape[0]
    slot_iota = jnp.arange(slot_count, dtype=jnp.int32)
    same = slot_expert[:, None] == slot_expert[None, :]
    copy_of = jnp.sum((same & (slot_iota[None, :] < slot_iota[:, None])).astype(jnp.int32), axis=1)
    first_rank = (copy_of[:, None] * CAP + jnp.arange(CAP, dtype=jnp.int32)[None, :]).reshape(-1)
    usable = jnp.repeat(copy_of < 2, CAP)
    column_expert = jnp.repeat(slot_expert, CAP)
    named = jnp.zeros((tok_rows, slot_count * CAP), jnp.bool_)
    gate = jnp.zeros((tok_rows, slot_count * CAP), jnp.int32)
    for k in range(topk_count):
        hit = expert_ids[:, k : k + 1] == column_expert[None, :]
        named = named | hit
        gate = jnp.where(hit, gate_fixed[:, k : k + 1], gate)
    token_iota = jnp.arange(tok_rows, dtype=jnp.int32)
    earlier = (token_iota[:, None] > token_iota[None, :]).astype(BF)
    before = jnp.dot(earlier, named.astype(BF), preferred_element_type=F32).astype(jnp.int32)
    served = named & usable[None, :] & (before == first_rank[None, :])
    gate = jnp.where(served, gate, 0)
    high = (gate // 256).astype(F32) * (256.0 * gate_scale)
    low = (gate % 256).astype(F32) * gate_scale
    return served.astype(BF), high.astype(BF), low.astype(BF)


def solution(mesh):
    tensor_size = mesh.shape["tensor"]
    dp_size = mesh.shape["dp"]

    def shards(
        hidden, expert_ids, gate_fixed, slot_expert, expert_in, expert_out, shared_in, shared_out
    ):
        tok_rows, half_width = hidden.shape
        slot_count = slot_expert.shape[0]
        part = tok_rows // CHUNKS
        pieces = [
            lax.all_gather(hidden[c * part : (c + 1) * part], "dp", axis=0, tiled=True)
            for c in range(CHUNKS)
        ]
        served, high, low = slot_plan(expert_ids, gate_fixed, slot_expert)
        send_rows = lax.dot_general(
            served, hidden, (((0,), (0,)), ((), ())), preferred_element_type=F32
        ).astype(BF)
        arrived = lax.all_to_all(
            send_rows.reshape(slot_count, CAP, half_width),
            ("dp", "expert"),
            split_axis=0,
            concat_axis=0,
            tiled=True,
        )
        rows = arrived.reshape(-1, half_width)
        w_in = expert_in[0].reshape(half_width, -1)
        s_in = shared_in.reshape(half_width, -1)
        ff_e = w_in.shape[1] // 2
        ff_s = s_in.shape[1] // 2
        partial = jnp.dot(rows, w_in, preferred_element_type=F32)
        pieces[0], s_in, partial = lax.optimization_barrier((pieces[0], s_in, partial))
        pre = across_tensor(partial, tensor_size)
        routed_act = swiglu(pre[:, :ff_e], pre[:, ff_e:])
        answers = jnp.dot(routed_act, expert_out[0], preferred_element_type=F32).astype(BF)

        sums = []
        for c in range(CHUNKS):
            pre = across_tensor(jnp.dot(pieces[c], s_in, preferred_element_type=F32), tensor_size)
            act = swiglu(pre[:, :ff_s], pre[:, ff_s:])
            part_out = jnp.dot(act, shared_out, preferred_element_type=F32).astype(BF)
            sums.append(lax.psum_scatter(part_out, "dp", scatter_dimension=0, tiled=True))
        returned = lax.all_to_all(
            answers.reshape(slot_count, CAP, half_width),
            ("dp", "expert"),
            split_axis=0,
            concat_axis=0,
            tiled=True,
        ).reshape(-1, half_width)
        routed = jnp.dot(high, returned, preferred_element_type=F32) + jnp.dot(
            low, returned, preferred_element_type=F32
        )
        shared = jnp.concatenate(sums, axis=0).astype(F32)
        return (shared + routed).astype(BF)

    in_specs = (
        P(("dp", "expert"), "tensor"),
        P(("dp", "expert"), None),
        P(("dp", "expert"), None),
        P(),
        P(("dp", "expert"), "tensor", None, None),
        P(("dp", "expert"), None, "tensor"),
        P("tensor", None, "dp"),
        P("dp", "tensor"),
    )
    out_specs = P(("dp", "expert"), "tensor")
    return jax.shard_map(shards, mesh=mesh, in_specs=in_specs, out_specs=out_specs, check_vma=False)
```

```python
import jax
import jax.numpy as jnp
from jax import lax
from jax.sharding import PartitionSpec as P


CAP = 4
gate_scale = 1.0 / 65536.0
BF = jnp.bfloat16
F32 = jnp.float32


def swiglu(gate, up):
    return (jax.nn.silu(gate) * up).astype(BF)


def across_tensor(partial, tensor_size):
    sent = partial.astype(BF)
    total = partial
    for shift in range(1, tensor_size):
        ring = [(i, (i + shift) % tensor_size) for i in range(tensor_size)]
        total = total + lax.ppermute(sent, "tensor", ring).astype(F32)
    return total


def block_of(blocks, index):
    index = jnp.clip(index, 0, blocks.shape[0] - 1)
    return lax.dynamic_index_in_dim(blocks, index, axis=0, keepdims=False).astype(F32)


class LineScatter:

    def __init__(self, part_out, size):
        self.size = size
        self.blocks = part_out.reshape(size, -1, part_out.shape[1])
        self.me = lax.axis_index("dp")
        self.step = 0
        self.right = self.left = None
        self.got_right = self.got_left = None

    def sums(self):
        self.step += 1
        s, n = self.step, self.size
        right = block_of(self.blocks, n - s + self.me)
        left = block_of(self.blocks, self.me - (n - s))
        if s > 1:
            right = right + self.got_right.astype(F32)
            left = left + self.got_left.astype(F32)
        self.right, self.left = lax.optimization_barrier((right.astype(BF), left.astype(BF)))

    def send(self):
        s, n = self.step, self.size
        self.got_right = lax.ppermute(self.right, "dp", [(i, i + 1) for i in range(s)])
        self.got_left = lax.ppermute(self.left, "dp", [(n - 1 - i, n - 2 - i) for i in range(s)])

    def result(self):
        while self.step < self.size - 1:
            self.sums()
            self.send()
        own = block_of(self.blocks, self.me)
        return own + self.got_right.astype(F32) + self.got_left.astype(F32)


def slot_plan(expert_ids, gate_fixed, slot_expert):
    tok_rows, topk_count = expert_ids.shape
    slot_count = slot_expert.shape[0]
    slot_iota = jnp.arange(slot_count, dtype=jnp.int32)
    same = slot_expert[:, None] == slot_expert[None, :]
    copy_of = jnp.sum((same & (slot_iota[None, :] < slot_iota[:, None])).astype(jnp.int32), axis=1)
    first_rank = (copy_of[:, None] * CAP + jnp.arange(CAP, dtype=jnp.int32)[None, :]).reshape(-1)
    usable = jnp.repeat(copy_of < 2, CAP)
    column_expert = jnp.repeat(slot_expert, CAP)
    named = jnp.zeros((tok_rows, slot_count * CAP), jnp.bool_)
    gate = jnp.zeros((tok_rows, slot_count * CAP), jnp.int32)
    for k in range(topk_count):
        hit = expert_ids[:, k : k + 1] == column_expert[None, :]
        named = named | hit
        gate = jnp.where(hit, gate_fixed[:, k : k + 1], gate)
    token_iota = jnp.arange(tok_rows, dtype=jnp.int32)
    earlier = (token_iota[:, None] > token_iota[None, :]).astype(BF)
    before = jnp.dot(earlier, named.astype(BF), preferred_element_type=F32).astype(jnp.int32)
    served = named & usable[None, :] & (before == first_rank[None, :])
    gate = jnp.where(served, gate, 0)
    high = (gate // 256).astype(F32) * (256.0 * gate_scale)
    low = (gate % 256).astype(F32) * gate_scale
    return served.astype(BF), high.astype(BF), low.astype(BF)


def solution(mesh):
    tensor_size = mesh.shape["tensor"]
    dp_size = mesh.shape["dp"]

    def shards(
        hidden, expert_ids, gate_fixed, slot_expert, expert_in, expert_out, shared_in, shared_out
    ):
        tok_rows, half_width = hidden.shape
        slot_count = slot_expert.shape[0]
        cut = tok_rows * 5 // 8
        first = lax.all_gather(hidden[:cut], "dp", axis=0, tiled=True)
        second = lax.all_gather(hidden[cut:], "dp", axis=0, tiled=True)
        served, high, low = slot_plan(expert_ids, gate_fixed, slot_expert)
        send_rows = lax.dot_general(
            served, hidden, (((0,), (0,)), ((), ())), preferred_element_type=F32
        ).astype(BF)
        arrived = lax.all_to_all(
            send_rows.reshape(slot_count, CAP, half_width),
            ("dp", "expert"),
            split_axis=0,
            concat_axis=0,
            tiled=True,
        )
        rows = arrived.reshape(-1, half_width)
        w_in = expert_in[0].reshape(half_width, -1)
        s_in = shared_in.reshape(half_width, -1)
        ff_e = w_in.shape[1] // 2
        ff_s = s_in.shape[1] // 2
        partial = jnp.dot(rows, w_in, preferred_element_type=F32)
        pre = across_tensor(partial, tensor_size)
        routed_act = swiglu(pre[:, :ff_e], pre[:, ff_e:])
        answers = jnp.dot(routed_act, expert_out[0], preferred_element_type=F32).astype(BF)

        first, s_in, _ = lax.optimization_barrier((first, s_in, answers))

        def shared_part(tokens):
            partial = jnp.dot(tokens, s_in, preferred_element_type=F32)
            partial = lax.optimization_barrier(partial)
            pre = across_tensor(partial, tensor_size)
            act = swiglu(pre[:, :ff_s], pre[:, ff_s:])
            return jnp.dot(act, shared_out, preferred_element_type=F32).astype(BF)

        back = lax.all_to_all(
            answers.reshape(slot_count, CAP, half_width),
            ("dp", "expert"),
            split_axis=0,
            concat_axis=0,
            tiled=True,
        )
        line = LineScatter(shared_part(first), dp_size)
        for _ in range(min(2, dp_size - 1)):
            if line.step:
                line.send()
            line.sums()
        second, _, _ = lax.optimization_barrier((second, line.right, line.left))
        line.send()
        tail = lax.psum_scatter(shared_part(second), "dp", scatter_dimension=0, tiled=True)
        returned = back.reshape(-1, half_width)
        routed = jnp.dot(high, returned, preferred_element_type=F32) + jnp.dot(
            low, returned, preferred_element_type=F32
        )
        shared = jnp.concatenate([line.result(), tail.astype(F32)], axis=0)
        return (shared + routed).astype(BF)

    in_specs = (
        P(("dp", "expert"), "tensor"),
        P(("dp", "expert"), None),
        P(("dp", "expert"), None),
        P(),
        P(("dp", "expert"), "tensor", None, None),
        P(("dp", "expert"), None, "tensor"),
        P("tensor", None, "dp"),
        P("dp", "tensor"),
    )
    out_specs = P(("dp", "expert"), "tensor")

    return jax.shard_map(shards, mesh=mesh, in_specs=in_specs, out_specs=out_specs, check_vma=False)
```
